32 devices in a mesh: groups: 2 (over y), rows: 4 (over z), cols: 2 (over x), sub: 2 (over core).
Axes of the slice: x: 2, y: 2, z: 4, core: 2. Of those that a mesh axis runs over, the one named last changes fastest.
Arguments:
- returns: float32 [8, 64, 8192], P('groups', 'rows', ('cols', 'sub')), parts along dimension 0, may hold values from -6 to 6
- starts: int32 [8, 8192], P('groups', ('cols', 'sub')), parts along dimension 0, may hold values from 0 to 32
- start_block: float32 [8, 32, 8192], P('groups', None, ('cols', 'sub')), parts along dimension 0, may hold values from -6 to 6
Outputs:
- loadings: float32 [8, 32, 8192], P('groups', None, ('cols', 'sub')), parts along dimension 0
The draws below stay inside these ranges and needn't reach their ends.
There are 2 independent parts, one for each index of `groups`. The reference program is written for one: setup_inputs(seed, part) draws one part's arguments, and reference() takes and returns one part's arrays. A program takes and returns all parts, laid end to end along the dimension named above; each array names one. Nothing has to cross between parts.
Inputs may be any that keep to these rules, and one draw needn't show every extreme that they name: `starts`: days before an asset's start day hold returns that do not count.
All inputs are finite; a program needn't handle non-finite values.
Results may differ from the reference program's by a relative error of at most 0.0078.
Values may be sent and summed in bfloat16 or wider, within the bound.
A program may use at most 64 MiB of HBM per device.

```python
import jax
import jax.numpy as jnp
from jax import lax

ASSETS = 8192
K = 32
ITERS = 3
NWIN = 4
TIME = 64


def place_ends(array, rng, low, top_value):
    dims = array.shape
    index_at = [jax.random.randint(jax.random.fold_in(rng, axis), (), 0, dims[axis]) for axis in range(len(dims))]
    array = array.at[tuple(index_at)].set(low)
    longest = dims.index(max(dims))
    index_at[longest] = (index_at[longest] + 1) % dims[longest]
    return array.at[tuple(index_at)].set(top_value)


def block_scale(own_key, extent, cuts, least, high):
    def one(dim, parts):
        heights = jax.random.uniform(jax.random.fold_in(jax.random.fold_in(own_key, 6), dim), (parts,), jnp.float32, least / len(cuts), high / len(cuts))
        return jnp.repeat(jnp.exp(heights), extent[dim] // parts).reshape((-1,) + (1,) * (len(extent) - dim - 1))

    gain = one(*cuts[0])
    for cut in cuts[1:]:
        gain = gain * one(*cut)
    return gain


def noise(own_key, shape, width, limit, shards=(), kind=jnp.bfloat16):
    level = block_scale(own_key, shape, shards, -0.22, 0.18) if shards else 1.0
    array = jax.random.normal(own_key, shape, jnp.float32) * width * level
    return jnp.minimum(jnp.maximum(array, -limit), limit).astype(kind)


def setup_inputs(seed: int = 0, part: int = 0) -> dict:
    key_list = jax.random.split(jax.random.key(seed), 4)
    own_keys = jax.random.split(jax.random.fold_in(key_list[3], part), 4)
    returns = noise(own_keys[0], (NWIN, TIME, ASSETS), 1.0, 6.0, ((1, 4), (2, 4)), jnp.float32)
    starts = place_ends(jax.random.randint(own_keys[1], (NWIN, ASSETS), 0, TIME // 2 + 1), jax.random.fold_in(own_keys[1], 1), 0, (TIME // 2 + 1) - 1).astype(jnp.int32)
    start_block = noise(own_keys[2], (NWIN, K, ASSETS), 1.0, 6.0, ((2, 4),), jnp.float32)
    return dict(returns=returns, starts=starts, start_block=start_block)


def standardize(returns, starts):
    days = jnp.arange(TIME, dtype=jnp.int32)
    live = (days[None, :, None] >= starts[:, None, :]).astype(jnp.float32)
    counts = (TIME - starts).astype(jnp.float32)
    mean = lax.optimization_barrier(jnp.sum(live * returns, axis=1)) / counts
    centered = live * (returns - mean[:, None, :])
    squares = lax.optimization_barrier(jnp.sum(centered * centered, axis=1))
    return (centered * lax.rsqrt(squares + 1.0)[:, None, :]).astype(jnp.bfloat16)

def one_window(pair):
    scaled, factors = pair
    widened = scaled.astype(jnp.float32)
    for step in range(ITERS):
        rounded = factors.astype(jnp.bfloat16)
        proj = jnp.dot(rounded.astype(jnp.float32), scaled.T.astype(jnp.float32), preferred_element_type=jnp.float32)
        image = jnp.dot(proj, widened, precision=lax.Precision.HIGHEST)
        gram = jnp.dot(image, image.T, precision=lax.Precision.HIGHEST) / ASSETS
        lower = jnp.linalg.cholesky(gram)
        factors = jax.scipy.linalg.solve_triangular(lower, image, lower=True)
    return factors

def reference(returns, starts, start_block):
    scaled = standardize(returns, starts)
    return lax.map(one_window, (scaled, start_block))
```

```python
import functools

import jax
import jax.numpy as jnp
from jax import lax
from jax.experimental import pallas as pl
from jax.experimental.pallas import tpu as pltpu
from jax.sharding import PartitionSpec as P

ITERS = 3
HIGHEST = lax.Precision.HIGHEST
MESH = pl.DeviceIdType.MESH
NT = (((1,), (1,)), ((), ()))
SUBLANES = 8


def eliminate(gram, right):
    size = gram.shape[0]
    height = min(SUBLANES, size)
    blocks = size // height
    gs = [gram[b * height:(b + 1) * height] for b in range(blocks)]
    rs = [right[b * height:(b + 1) * height] for b in range(blocks)]
    row_id = lax.broadcasted_iota(jnp.int32, (height, 1), 0)
    diag = [jnp.ones((height, 1), jnp.float32) for _ in range(blocks)]
    for j in range(size):
        b, i = divmod(j, height)
        grow = gs[b][i:i + 1]
        rrow = rs[b][i:i + 1]
        pivot = gs[b][i:i + 1, j:j + 1]
        diag[b] = jnp.where(row_id == i, pivot, diag[b])
        inverse = 1.0 / pivot
        for c in range(b, blocks):
            factor = gs[c][:, j:j + 1] * inverse
            if c == b:
                factor = jnp.where(row_id > i, factor, 0.0)
            gs[c] = gs[c] - factor * grow
            rs[c] = rs[c] - factor * rrow
    return jnp.concatenate([r * lax.rsqrt(d) for r, d in zip(rs, diag)], axis=0)


def kernel(rows, cols, subs, assets,
           returns_ref, starts_ref, start_ref, out_ref,
           xbuf, sbuf, part, rs, mine, quad, mloc, mall,
           xs, xr, ss, sr, ps, pr, qs, qr, ms, mr):
    r = lax.axis_index("rows")
    mates = cols * subs
    m = lax.axis_index("cols") * subs + lax.axis_index("sub")
    windows, days, width = returns_ref.shape
    k = start_ref.shape[1]
    total = days * rows
    own = width // rows

    def row_peer(d):
        return lax.rem(r + d, rows)

    def mate(d):
        return lax.rem(m + d, mates)

    def row_id(q):
        return {"rows": q}

    def mate_id(q):
        return {"cols": q // subs, "sub": lax.rem(q, subs)}

    def columns(q):
        return pl.ds(pl.multiple_of(q * own, own), own)

    barrier = pltpu.get_barrier_semaphore()
    for d in range(1, rows):
        pl.semaphore_signal(barrier, inc=1, device_id=row_id(row_peer(d)), device_id_type=MESH)
    for d in range(1, mates):
        pl.semaphore_signal(barrier, inc=1, device_id=mate_id(mate(d)), device_id_type=MESH)
    pl.semaphore_wait(barrier, rows - 1 + mates - 1)

    def copy_to(src, dst, send, recv, target):
        return pltpu.make_async_remote_copy(
            src_ref=src, dst_ref=dst, send_sem=send, recv_sem=recv,
            device_id=target, device_id_type=MESH)

    sends = []
    for w in range(windows):
        for d in range(1, rows):
            q = row_peer(d)
            c = copy_to(returns_ref.at[w, :, columns(q)], xbuf.at[r, w], xs.at[w, d],
                        xr.at[w, r], row_id(q))
            c.start()
            sends.append(c)
    xbuf[r] = returns_ref[:, :, columns(r)]

    day = lax.broadcasted_iota(jnp.int32, (total, own), 0)
    for w in range(windows):
        for d in range(1, rows):
            q = row_peer(d)
            copy_to(returns_ref.at[w, :, columns(q)], xbuf.at[q, w], xs.at[w, d],
                    xr.at[w, q], row_id(q)).wait_recv()
        x = jnp.concatenate([xbuf[q, w] for q in range(rows)], axis=0)
        begin = starts_ref[pl.ds(w, 1), columns(r)]
        live = day >= begin
        counts = (total - begin).astype(jnp.float32)
        mean = jnp.sum(jnp.where(live, x, 0.0), axis=0, keepdims=True) / counts
        centered = jnp.where(live, x - mean, 0.0)
        squares = jnp.sum(centered * centered, axis=0, keepdims=True)
        scaled = (centered * lax.rsqrt(squares + 1.0)).astype(jnp.bfloat16)
        sbuf[r, w] = scaled
        first = start_ref[w, :, columns(r)].astype(jnp.bfloat16)
        part[w] = lax.dot_general(jnp.concatenate([first, scaled], axis=0), scaled, NT,
                                  preferred_element_type=jnp.float32)

    for d in range(1, rows):
        q = row_peer(d)
        c = copy_to(part.at[q], rs.at[r], ps.at[d], pr.at[r], row_id(q))
        c.start()
        sends.append(c)
    for d in range(1, rows):
        q = row_peer(d)
        c = copy_to(sbuf.at[r], sbuf.at[r], ss.at[d], sr.at[r], row_id(q))
        c.start()
        sends.append(c)
    rs[r] = part[r]
    for d in range(1, rows):
        q = row_peer(d)
        copy_to(part.at[q], rs.at[q], ps.at[d], pr.at[q], row_id(q)).wait_recv()
    summed = rs[0]
    for q in range(1, rows):
        summed = summed + rs[q]
    mine[...] = summed
    for d in range(1, mates):
        q = mate(d)
        c = copy_to(mine, quad.at[m], qs.at[d], qr.at[m], mate_id(q))
        c.start()
        sends.append(c)
    quad[m] = summed
    for d in range(1, mates):
        q = mate(d)
        copy_to(mine, quad.at[q], qs.at[d], qr.at[q], mate_id(q)).wait_recv()
    both = quad[0]
    for q in range(1, mates):
        both = both + quad[q]
    proj, corr = both[:k], both[k:]
    for step in range(ITERS):
        image = jnp.dot(proj, corr, precision=HIGHEST, preferred_element_type=jnp.float32)
        gram = lax.dot_general(image, proj, NT, precision=HIGHEST,
                               preferred_element_type=jnp.float32) / assets
        proj = eliminate(gram, image if step < ITERS - 1 else proj)
    mloc[...] = proj
    for d in range(1, rows):
        q = row_peer(d)
        c = copy_to(mloc, mall.at[r], ms.at[d], mr.at[r], row_id(q))
        c.start()
        sends.append(c)
    mall[r] = proj
    for d in range(1, rows):
        q = row_peer(d)
        copy_to(mloc, mall.at[q], ms.at[d], mr.at[q], row_id(q)).wait_recv()
    stacked = []
    for w in range(windows):
        value = mall[w]
        high = value.astype(jnp.bfloat16)
        low = (value - high.astype(jnp.float32)).astype(jnp.bfloat16)
        stacked.append(jnp.concatenate([high, low], axis=0))

    def finish(q):
        for w in range(windows):
            wide = jnp.dot(stacked[w], sbuf[q, w], preferred_element_type=jnp.float32)
            out_ref[w, :, columns(q)] = wide[:k] + wide[k:]

    finish(r)
    for d in range(1, rows):
        q = row_peer(d)
        copy_to(sbuf.at[q], sbuf.at[q], ss.at[d], sr.at[q], row_id(q)).wait_recv()
        finish(q)
    for c in sends:
        c.wait_send()


def fused(returns, starts, start_block, rows, cols, subs):
    windows, days, width = returns.shape
    k = start_block.shape[1]
    total = days * rows
    own = width // rows
    mates = cols * subs
    f32 = jnp.float32
    dma = pltpu.SemaphoreType.DMA
    return pl.pallas_call(
        functools.partial(kernel, rows, cols, subs, width * mates),
        out_shape=jax.ShapeDtypeStruct(start_block.shape, f32),
        in_specs=[pl.BlockSpec(memory_space=pltpu.VMEM)] * 3,
        out_specs=pl.BlockSpec(memory_space=pltpu.VMEM),
        scratch_shapes=[
            pltpu.VMEM((rows, windows, days, own), f32),
            pltpu.VMEM((rows, windows, total, own), jnp.bfloat16),
            pltpu.VMEM((windows, k + total, total), f32),
            pltpu.VMEM((rows, k + total, total), f32),
            pltpu.VMEM((k + total, total), f32),
            pltpu.VMEM((mates, k + total, total), f32),
            pltpu.VMEM((k, total), f32),
            pltpu.VMEM((windows, k, total), f32),
            dma((windows, rows)), dma((windows, rows)),
            dma((rows,)), dma((rows,)),
            dma((rows,)), dma((rows,)),
            dma((mates,)), dma((mates,)),
            dma((rows,)), dma((rows,)),
        ],
        compiler_params=pltpu.CompilerParams(collective_id=0, has_side_effects=True),
    )(returns, starts, start_block)


def gram_of(image):
    return jnp.einsum("wkj,wlj->wkl", image, image, precision=HIGHEST)


def project(factors, scaled):
    rounded = factors.astype(jnp.bfloat16)
    return jnp.einsum("wka,wta->wkt", rounded, scaled, preferred_element_type=jnp.float32)


def expand(proj, widened):
    return jnp.einsum("wkt,wta->wka", proj, widened, precision=HIGHEST)


def orthonormal(image, gram, assets):
    lower = jnp.linalg.cholesky(gram / assets)
    return jax.scipy.linalg.solve_triangular(lower, image, lower=True)


def stepwise(returns, starts, start_block, rows, mates):
    windows, days, width = returns.shape
    row_pos = lax.axis_index("rows")
    total_days = days * rows
    day_index = row_pos * days + jnp.arange(days, dtype=jnp.int32)
    live = (day_index[None, :, None] >= starts[:, None, :]).astype(jnp.float32)
    counts = (total_days - starts).astype(jnp.float32)
    masked = live * returns
    sums = lax.psum(jnp.sum(masked, axis=1), "rows")
    mean = sums / counts
    centered = live * (returns - mean[:, None, :])
    squares = lax.psum(jnp.sum(centered * centered, axis=1), "rows")
    scaled = (centered * lax.rsqrt(squares + 1.0)[:, None, :]).astype(jnp.bfloat16)
    widened = scaled.astype(jnp.float32)
    factors = start_block
    for step in range(ITERS):
        proj = lax.psum(project(factors, scaled), ("cols", "sub"))
        image = lax.psum(expand(proj, widened), "rows")
        gram = lax.psum(gram_of(image), ("cols", "sub"))
        factors = orthonormal(image, gram, width * mates)
    return factors


def on_device(rows, cols, subs, returns, starts, start_block):
    windows, days, width = returns.shape
    k = start_block.shape[1]
    fits = (windows == rows and width % (128 * rows) == 0 and days % 8 == 0 and k % 16 == 0
            and days * rows <= 128 and rows > 1 and cols * subs > 1)
    if fits:
        return fused(returns, starts, start_block, rows, cols, subs)
    return stepwise(returns, starts, start_block, rows, cols * subs)


def solution(mesh):
    placed = (
        P("groups", "rows", ("cols", "sub")),
        P("groups", ("cols", "sub")),
        P("groups", None, ("cols", "sub")),
    )
    sizes = (mesh.shape["rows"], mesh.shape["cols"], mesh.shape["sub"])
    return jax.shard_map(
        functools.partial(on_device, *sizes),
        mesh=mesh,
        in_specs=placed,
        out_specs=P("groups", None, ("cols", "sub")),
        check_vma=False,
    )
```

```python
import functools

import jax
import jax.numpy as jnp
from jax import lax
from jax.experimental import pallas as pl
from jax.experimental.pallas import tpu as pltpu
from jax.sharding import PartitionSpec as P

ITERS = 3
HIGHEST = lax.Precision.HIGHEST
MESH = pl.DeviceIdType.MESH
NT = (((1,), (1,)), ((), ()))
SUBLANES = 8


def eliminate(gram, right):
    size = gram.shape[0]
    height = min(SUBLANES, size)
    blocks = size // height
    gs = [gram[b * height:(b + 1) * height] for b in range(blocks)]
    rs = [right[b * height:(b + 1) * height] for b in range(blocks)]
    row_id = lax.broadcasted_iota(jnp.int32, (height, 1), 0)
    diag = [jnp.ones((height, 1), jnp.float32) for _ in range(blocks)]
    for j in range(size):
        b, i = divmod(j, height)
        grow = gs[b][i:i + 1]
        rrow = rs[b][i:i + 1]
        pivot = gs[b][i:i + 1, j:j + 1]
        diag[b] = jnp.where(row_id == i, pivot, diag[b])
        inverse = 1.0 / pivot
        for c in range(b, blocks):
            factor = gs[c][:, j:j + 1] * inverse
            if c == b:
                factor = jnp.where(row_id > i, factor, 0.0)
            gs[c] = gs[c] - factor * grow
            rs[c] = rs[c] - factor * rrow
    return jnp.concatenate([r * lax.rsqrt(d) for r, d in zip(rs, diag)], axis=0)


def kernel(rows, cols, subs, assets,
           returns_ref, starts_ref, start_ref, out_ref,
           held, begins, firsts, obuf, xbuf, sbuf, part, rs, mine, quad, mloc, mall,
           ls, bs, os, xs, xr, to_right, to_left, sr, ps, pr, qs, qr, ms, mr):
    r = lax.axis_index("rows")
    mates = cols * subs
    m = lax.axis_index("cols") * subs + lax.axis_index("sub")
    windows, days, width = returns_ref.shape
    k = start_ref.shape[1]
    total = days * rows
    own = width // rows
    half = (k + total) // 2

    def row_peer(d):
        return lax.rem(r + d, rows)

    def mate(d):
        return lax.rem(m + d, mates)

    def row_id(q):
        return {"rows": q}

    def mate_id(q):
        return {"cols": q // subs, "sub": lax.rem(q, subs)}

    def columns(q):
        return pl.ds(pl.multiple_of(q * own, own), own)

    loads = [pltpu.make_async_copy(returns_ref.at[w], held.at[w], ls.at[w]) for w in range(windows)]
    for c in loads:
        c.start()
    load_begins = pltpu.make_async_copy(starts_ref.at[:, columns(r)], begins, bs.at[0])
    load_begins.start()
    load_firsts = pltpu.make_async_copy(start_ref.at[:, :, columns(r)], firsts, bs.at[1])
    load_firsts.start()

    barrier = pltpu.get_barrier_semaphore()
    for d in range(1, rows):
        pl.semaphore_signal(barrier, inc=1, device_id=row_id(row_peer(d)), device_id_type=MESH)
    for d in range(1, mates):
        pl.semaphore_signal(barrier, inc=1, device_id=mate_id(mate(d)), device_id_type=MESH)
    pl.semaphore_wait(barrier, rows - 1 + mates - 1)

    def copy_to(src, dst, send, recv, target):
        return pltpu.make_async_remote_copy(
            src_ref=src, dst_ref=dst, send_sem=send, recv_sem=recv,
            device_id=target, device_id_type=MESH)

    sends = []
    for w in range(windows):
        loads[w].wait()
        for d in range(1, rows):
            q = row_peer(d)
            c = copy_to(held.at[w, :, columns(q)], xbuf.at[r, w], xs.at[w, d],
                        xr.at[w, r], row_id(q))
            c.start()
            sends.append(c)
    xbuf[r] = held[:, :, columns(r)]
    load_begins.wait()
    load_firsts.wait()

    day = lax.broadcasted_iota(jnp.int32, (total, own), 0)
    for w in range(windows):
        for d in range(1, rows):
            q = row_peer(d)
            copy_to(held.at[w, :, columns(q)], xbuf.at[q, w], xs.at[w, d],
                    xr.at[w, q], row_id(q)).wait_recv()
        x = jnp.concatenate([xbuf[q, w] for q in range(rows)], axis=0)
        begin = begins[w:w + 1]
        live = day >= begin
        counts = (total - begin).astype(jnp.float32)
        mean = jnp.sum(jnp.where(live, x, 0.0), axis=0, keepdims=True) / counts
        centered = jnp.where(live, x - mean, 0.0)
        squares = jnp.sum(centered * centered, axis=0, keepdims=True)
        scaled = (centered * lax.rsqrt(squares + 1.0)).astype(jnp.bfloat16)
        sbuf[r, w] = scaled
        first = firsts[w].astype(jnp.bfloat16)
        sums = lax.dot_general(jnp.concatenate([first, scaled], axis=0), scaled, NT,
                               preferred_element_type=jnp.float32)
        part[w] = jnp.concatenate([sums[:half], sums[half:]], axis=1)

    for d in range(1, rows):
        q = row_peer(d)
        c = copy_to(part.at[q], rs.at[r], ps.at[d], pr.at[r], row_id(q))
        c.start()
        sends.append(c)

    def hop(q, w, right):
        sem = to_right if right else to_left
        target = row_id(lax.rem(r + (1 if right else rows - 1), rows))
        return copy_to(sbuf.at[q, w], sbuf.at[q, w], sem.at[q, w], sr.at[q, w], target)

    def hops(t, some, act):
        right_block = lax.rem(r - t + rows, rows)
        left_block = lax.rem(r + t, rows)
        for w in some:
            @pl.when(jnp.logical_and(r - t >= 0, r < rows - 1))
            def _():
                act(hop(right_block, w, True), t > 0)

            @pl.when(jnp.logical_and(r + t < rows, r > 0))
            def _():
                act(hop(left_block, w, False), t > 0)

    def forward(t, some):
        for w in some:
            if t > 0:
                @pl.when(r - t >= 0)
                def _():
                    hop(lax.rem(r - t + rows, rows), w, True).wait_recv()

                @pl.when(r + t < rows)
                def _():
                    hop(lax.rem(r + t, rows), w, True).wait_recv()
            hops(t, (w,), lambda c, _: c.start())

    early, late = range(windows // 2), range(windows // 2, windows)
    schedule = [(t, some) for t in range(1, rows) for some in (early, late)]
    forward(0, range(windows))
    rs[r] = part[r]
    for d in range(1, rows):
        q = row_peer(d)
        copy_to(part.at[q], rs.at[q], ps.at[d], pr.at[q], row_id(q)).wait_recv()
    forward(*schedule.pop(0))
    summed = rs[0]
    for q in range(1, rows):
        summed = summed + rs[q]
    mine[...] = summed
    for d in range(1, mates):
        q = mate(d)
        c = copy_to(mine, quad.at[m], qs.at[d], qr.at[m], mate_id(q))
        c.start()
        sends.append(c)
    quad[m] = summed
    for d in range(1, mates):
        q = mate(d)
        copy_to(mine, quad.at[q], qs.at[d], qr.at[q], mate_id(q)).wait_recv()
    forward(*schedule.pop(0))
    both = quad[0]
    for q in range(1, mates):
        both = both + quad[q]
    both = jnp.concatenate([both[:, :total], both[:, total:]], axis=0)
    proj, corr = both[:k], both[k:]
    for step in range(ITERS):
        if step > 0 and len(schedule) > 2:
            forward(*schedule.pop(0))
        image = jnp.dot(proj, corr, precision=HIGHEST, preferred_element_type=jnp.float32)
        gram = lax.dot_general(image, proj, NT, precision=HIGHEST,
                               preferred_element_type=jnp.float32) / assets
        proj = eliminate(gram, image if step < ITERS - 1 else proj)
    mloc[...] = proj
    for d in range(1, rows):
        q = row_peer(d)
        c = copy_to(mloc, mall.at[r], ms.at[d], mr.at[r], row_id(q))
        c.start()
        sends.append(c)
    mall[r] = proj
    for entry in schedule:
        forward(*entry)
    for d in range(1, rows):
        q = row_peer(d)
        copy_to(mloc, mall.at[q], ms.at[d], mr.at[q], row_id(q)).wait_recv()
    stacked = []
    for w in range(windows):
        value = mall[w]
        high = value.astype(jnp.bfloat16)
        low = (value - high.astype(jnp.float32)).astype(jnp.bfloat16)
        stacked.append(jnp.concatenate([high, low], axis=0))

    def finish(q):
        for w in range(windows):
            wide = jnp.dot(stacked[w], sbuf[q, w], preferred_element_type=jnp.float32)
            obuf[q, w] = wide[:k] + wide[k:]
        c = pltpu.make_async_copy(obuf.at[q], out_ref.at[:, :, columns(q)], os.at[q])
        c.start()

    finish(r)
    for t in range(1, rows):
        for near in (True, False):
            @pl.when(r - t >= 0 if near else r + t < rows)
            def _():
                q = lax.rem(r - t + rows if near else r + t, rows)
                finish(q)
    for c in sends:
        c.wait_send()
    for t in range(rows):
        hops(t, range(windows), lambda c, _: c.wait_send())
    for q in range(rows):
        pltpu.make_async_copy(obuf.at[q], out_ref.at[:, :, columns(q)], os.at[q]).wait()


def fused(returns, starts, start_block, rows, cols, subs):
    windows, days, width = returns.shape
    k = start_block.shape[1]
    total = days * rows
    own = width // rows
    mates = cols * subs
    half = (k + total) // 2
    f32 = jnp.float32
    dma = pltpu.SemaphoreType.DMA
    return pl.pallas_call(
        functools.partial(kernel, rows, cols, subs, width * mates),
        out_shape=jax.ShapeDtypeStruct(start_block.shape, f32),
        in_specs=[pl.BlockSpec(memory_space=pl.ANY)] * 3,
        out_specs=pl.BlockSpec(memory_space=pl.ANY),
        scratch_shapes=[
            pltpu.VMEM(returns.shape, f32),
            pltpu.VMEM((windows, own), jnp.int32),
            pltpu.VMEM((windows, k, own), f32),
            pltpu.VMEM((rows, windows, k, own), f32),
            pltpu.VMEM((rows, windows, days, own), f32),
            pltpu.VMEM((rows, windows, total, own), jnp.bfloat16),
            pltpu.VMEM((windows, half, 2 * total), f32),
            pltpu.VMEM((rows, half, 2 * total), f32),
            pltpu.VMEM((half, 2 * total), f32),
            pltpu.VMEM((mates, half, 2 * total), f32),
            pltpu.VMEM((k, total), f32),
            pltpu.VMEM((windows, k, total), f32),
            dma((windows,)), dma((2,)), dma((rows,)),
            dma((windows, rows)), dma((windows, rows)),
            dma((rows, windows)), dma((rows, windows)), dma((rows, windows)),
            dma((rows,)), dma((rows,)),
            dma((mates,)), dma((mates,)),
            dma((rows,)), dma((rows,)),
        ],
        compiler_params=pltpu.CompilerParams(collective_id=0, has_side_effects=True),
    )(returns, starts, start_block)


def gram_of(image):
    return jnp.einsum("wkj,wlj->wkl", image, image, precision=HIGHEST)


def project(factors, scaled):
    rounded = factors.astype(jnp.bfloat16)
    return jnp.einsum("wka,wta->wkt", rounded, scaled, preferred_element_type=jnp.float32)


def expand(proj, widened):
    return jnp.einsum("wkt,wta->wka", proj, widened, precision=HIGHEST)


def orthonormal(image, gram, assets):
    lower = jnp.linalg.cholesky(gram / assets)
    return jax.scipy.linalg.solve_triangular(lower, image, lower=True)


def stepwise(returns, starts, start_block, rows, mates):
    windows, days, width = returns.shape
    row_pos = lax.axis_index("rows")
    total_days = days * rows
    day_index = row_pos * days + jnp.arange(days, dtype=jnp.int32)
    live = (day_index[None, :, None] >= starts[:, None, :]).astype(jnp.float32)
    counts = (total_days - starts).astype(jnp.float32)
    masked = live * returns
    sums = lax.psum(jnp.sum(masked, axis=1), "rows")
    mean = sums / counts
    centered = live * (returns - mean[:, None, :])
    squares = lax.psum(jnp.sum(centered * centered, axis=1), "rows")
    scaled = (centered * lax.rsqrt(squares + 1.0)[:, None, :]).astype(jnp.bfloat16)
    widened = scaled.astype(jnp.float32)
    factors = start_block
    for step in range(ITERS):
        proj = lax.psum(project(factors, scaled), ("cols", "sub"))
        image = lax.psum(expand(proj, widened), "rows")
        gram = lax.psum(gram_of(image), ("cols", "sub"))
        factors = orthonormal(image, gram, width * mates)
    return factors


def on_device(rows, cols, subs, returns, starts, start_block):
    windows, days, width = returns.shape
    k = start_block.shape[1]
    fits = (windows == rows and width % (128 * rows) == 0 and days % 8 == 0 and k % 16 == 0
            and days * rows <= 64 and (days * rows + k) % 16 == 0 and rows > 1 and cols * subs > 1)
    if fits:
        return fused(returns, starts, start_block, rows, cols, subs)
    return stepwise(returns, starts, start_block, rows, cols * subs)


def solution(mesh):
    placed = (
        P("groups", "rows", ("cols", "sub")),
        P("groups", ("cols", "sub")),
        P("groups", None, ("cols", "sub")),
    )
    sizes = (mesh.shape["rows"], mesh.shape["cols"], mesh.shape["sub"])
    return jax.shard_map(
        functools.partial(on_device, *sizes),
        mesh=mesh,
        in_specs=placed,
        out_specs=P("groups", None, ("cols", "sub")),
        check_vma=False,
    )
```

```python
import functools

import jax
import jax.numpy as jnp
from jax import lax
from jax.experimental import pallas as pl
from jax.experimental.pallas import tpu as pltpu
from jax.sharding import PartitionSpec as P

ITERS = 3
HIGHEST = lax.Precision.HIGHEST
MESH = pl.DeviceIdType.MESH
NT = (((1,), (1,)), ((), ()))
SUBLANES = 8


def eliminate(gram, right):
    size = gram.shape[0]
    height = min(SUBLANES, size)
    blocks = size // height
    gs = [gram[b * height:(b + 1) * height] for b in range(blocks)]
    rs = [right[b * height:(b + 1) * height] for b in range(blocks)]
    row_id = lax.broadcasted_iota(jnp.int32, (height, 1), 0)
    diag = [jnp.ones((height, 1), jnp.float32) for _ in range(blocks)]
    for j in range(size):
        b, i = divmod(j, height)
        grow = gs[b][i:i + 1]
        rrow = rs[b][i:i + 1]
        pivot = gs[b][i:i + 1, j:j + 1]
        diag[b] = jnp.where(row_id == i, pivot, diag[b])
        inverse = 1.0 / pivot
        for c in range(b, blocks):
            factor = gs[c][:, j:j + 1] * inverse
            if c == b:
                factor = jnp.where(row_id > i, factor, 0.0)
            gs[c] = gs[c] - factor * grow
            rs[c] = rs[c] - factor * rrow
    return jnp.concatenate([r * lax.rsqrt(d) for r, d in zip(rs, diag)], axis=0)


def kernel(rows, cols, subs, assets,
           returns_ref, starts_ref, start_ref, out_ref,
           held, begins, firsts, obuf, xbuf, sbuf, part, rs, mine, quad, mloc, mall,
           ls, bs, os, xs, xr, to_right, to_left, sr, ps, pr, qs, qr, ms, mr):
    r = lax.axis_index("rows")
    mates = cols * subs
    m = lax.axis_index("cols") * subs + lax.axis_index("sub")
    windows, days, width = returns_ref.shape
    k = start_ref.shape[1]
    total = days * rows
    own = width // rows
    half = (k + total) // 2

    def row_peer(d):
        return lax.rem(r + d, rows)

    def mate(d):
        return lax.rem(m + d, mates)

    def row_id(q):
        return {"rows": q}

    def mate_id(q):
        return {"cols": q // subs, "sub": lax.rem(q, subs)}

    def columns(q):
        return pl.ds(pl.multiple_of(q * own, own), own)

    loads = [pltpu.make_async_copy(returns_ref.at[w], held.at[w], ls.at[w]) for w in range(windows)]
    for c in loads:
        c.start()
    load_begins = pltpu.make_async_copy(starts_ref.at[:, columns(r)], begins, bs.at[0])
    load_begins.start()
    load_firsts = pltpu.make_async_copy(start_ref.at[:, :, columns(r)], firsts, bs.at[1])
    load_firsts.start()

    barrier = pltpu.get_barrier_semaphore()
    for d in range(1, rows):
        pl.semaphore_signal(barrier, inc=1, device_id=row_id(row_peer(d)), device_id_type=MESH)
    for d in range(1, mates):
        pl.semaphore_signal(barrier, inc=1, device_id=mate_id(mate(d)), device_id_type=MESH)
    pl.semaphore_wait(barrier, rows - 1 + mates - 1)

    def copy_to(src, dst, send, recv, target):
        return pltpu.make_async_remote_copy(
            src_ref=src, dst_ref=dst, send_sem=send, recv_sem=recv,
            device_id=target, device_id_type=MESH)

    sends = []
    for w in range(windows):
        loads[w].wait()
        for d in range(1, rows):
            q = row_peer(d)
            c = copy_to(held.at[w, :, columns(q)], xbuf.at[r, w], xs.at[w, d],
                        xr.at[w, r], row_id(q))
            c.start()
            sends.append(c)
    xbuf[r] = held[:, :, columns(r)]
    load_begins.wait()
    load_firsts.wait()

    def hop(q, w, right):
        sem = to_right if right else to_left
        target = row_id(lax.rem(r + (1 if right else rows - 1), rows))
        return copy_to(sbuf.at[q, w], sbuf.at[q, w], sem.at[q, w], sr.at[q, w], target)

    def hops(t, some, act):
        right_block = lax.rem(r - t + rows, rows)
        left_block = lax.rem(r + t, rows)
        for w in some:
            @pl.when(jnp.logical_and(r - t >= 0, r < rows - 1))
            def _():
                act(hop(right_block, w, True), t > 0)

            @pl.when(jnp.logical_and(r + t < rows, r > 0))
            def _():
                act(hop(left_block, w, False), t > 0)

    def forward(t, some):
        for w in some:
            if t > 0:
                @pl.when(r - t >= 0)
                def _():
                    hop(lax.rem(r - t + rows, rows), w, True).wait_recv()

                @pl.when(r + t < rows)
                def _():
                    hop(lax.rem(r + t, rows), w, True).wait_recv()
            hops(t, (w,), lambda c, _: c.start())

    def deliver(w):
        return copy_to(part.at[w], rs.at[r], ps.at[w], pr.at[r], row_id(w))

    ahead = windows // 2
    day = lax.broadcasted_iota(jnp.int32, (total, own), 0)
    for w in range(windows):
        for d in range(1, rows):
            q = row_peer(d)
            copy_to(held.at[w, :, columns(q)], xbuf.at[q, w], xs.at[w, d],
                    xr.at[w, q], row_id(q)).wait_recv()
        x = jnp.concatenate([xbuf[q, w] for q in range(rows)], axis=0)
        begin = begins[w:w + 1]
        live = day >= begin
        counts = (total - begin).astype(jnp.float32)
        mean = jnp.sum(jnp.where(live, x, 0.0), axis=0, keepdims=True) / counts
        centered = jnp.where(live, x - mean, 0.0)
        squares = jnp.sum(centered * centered, axis=0, keepdims=True)
        scaled = (centered * lax.rsqrt(squares + 1.0)).astype(jnp.bfloat16)
        sbuf[r, w] = scaled
        first = firsts[w].astype(jnp.bfloat16)
        sums = lax.dot_general(jnp.concatenate([first, scaled], axis=0), scaled, NT,
                               preferred_element_type=jnp.float32)
        part[w] = jnp.concatenate([sums[:half], sums[half:]], axis=1)

        @pl.when(r != w)
        def _():
            deliver(w).start()

        if w < ahead:
            forward(0, (w,))


    early, late = range(windows // 2), range(windows // 2, windows)
    schedule = [(t, some) for t in range(1, rows) for some in (early, late)]
    forward(0, range(ahead, windows))
    rs[r] = part[r]
    for d in range(1, rows):
        q = row_peer(d)
        copy_to(part.at[q], rs.at[q], ps.at[q], pr.at[q], row_id(q)).wait_recv()
    forward(*schedule.pop(0))
    summed = rs[0]
    for q in range(1, rows):
        summed = summed + rs[q]
    mine[...] = summed
    for d in range(1, mates):
        q = mate(d)
        c = copy_to(mine, quad.at[m], qs.at[d], qr.at[m], mate_id(q))
        c.start()
        sends.append(c)
    quad[m] = summed
    for d in range(1, mates):
        q = mate(d)
        copy_to(mine, quad.at[q], qs.at[d], qr.at[q], mate_id(q)).wait_recv()
    forward(*schedule.pop(0))
    both = quad[0]
    for q in range(1, mates):
        both = both + quad[q]
    both = jnp.concatenate([both[:, :total], both[:, total:]], axis=0)
    proj, corr = both[:k], both[k:]
    for step in range(ITERS):
        if step > 0 and len(schedule) > 2:
            forward(*schedule.pop(0))
        image = jnp.dot(proj, corr, precision=HIGHEST, preferred_element_type=jnp.float32)
        gram = lax.dot_general(image, proj, NT, precision=HIGHEST,
                               preferred_element_type=jnp.float32) / assets
        proj = eliminate(gram, image if step < ITERS - 1 else proj)
    mloc[...] = proj
    for d in range(1, rows):
        q = row_peer(d)
        c = copy_to(mloc, mall.at[r], ms.at[d], mr.at[r], row_id(q))
        c.start()
        sends.append(c)
    mall[r] = proj
    for entry in schedule:
        forward(*entry)
    for d in range(1, rows):
        q = row_peer(d)
        copy_to(mloc, mall.at[q], ms.at[d], mr.at[q], row_id(q)).wait_recv()
    stacked = []
    for w in range(windows):
        value = mall[w]
        high = value.astype(jnp.bfloat16)
        low = (value - high.astype(jnp.float32)).astype(jnp.bfloat16)
        stacked.append(jnp.concatenate([high, low], axis=0))

    def finish(q):
        for w in range(windows):
            wide = jnp.dot(stacked[w], sbuf[q, w], preferred_element_type=jnp.float32)
            obuf[q, w] = wide[:k] + wide[k:]
        c = pltpu.make_async_copy(obuf.at[q], out_ref.at[:, :, columns(q)], os.at[q])
        c.start()

    finish(r)
    for t in range(1, rows):
        for near in (True, False):
            @pl.when(r - t >= 0 if near else r + t < rows)
            def _():
                q = lax.rem(r - t + rows if near else r + t, rows)
                finish(q)
    for c in sends:
        c.wait_send()
    for w in range(windows):
        @pl.when(r != w)
        def _():
            deliver(w).wait_send()
    for t in range(rows):
        hops(t, range(windows), lambda c, _: c.wait_send())
    for q in range(rows):
        pltpu.make_async_copy(obuf.at[q], out_ref.at[:, :, columns(q)], os.at[q]).wait()


def fused(returns, starts, start_block, rows, cols, subs):
    windows, days, width = returns.shape
    k = start_block.shape[1]
    total = days * rows
    own = width // rows
    mates = cols * subs
    half = (k + total) // 2
    f32 = jnp.float32
    dma = pltpu.SemaphoreType.DMA
    return pl.pallas_call(
        functools.partial(kernel, rows, cols, subs, width * mates),
        out_shape=jax.ShapeDtypeStruct(start_block.shape, f32),
        in_specs=[pl.BlockSpec(memory_space=pl.ANY)] * 3,
        out_specs=pl.BlockSpec(memory_space=pl.ANY),
        scratch_shapes=[
            pltpu.VMEM(returns.shape, f32),
            pltpu.VMEM((windows, own), jnp.int32),
            pltpu.VMEM((windows, k, own), f32),
            pltpu.VMEM((rows, windows, k, own), f32),
            pltpu.VMEM((rows, windows, days, own), f32),
            pltpu.VMEM((rows, windows, total, own), jnp.bfloat16),
            pltpu.VMEM((windows, half, 2 * total), f32),
            pltpu.VMEM((rows, half, 2 * total), f32),
            pltpu.VMEM((half, 2 * total), f32),
            pltpu.VMEM((mates, half, 2 * total), f32),
            pltpu.VMEM((k, total), f32),
            pltpu.VMEM((windows, k, total), f32),
            dma((windows,)), dma((2,)), dma((rows,)),
            dma((windows, rows)), dma((windows, rows)),
            dma((rows, windows)), dma((rows, windows)), dma((rows, windows)),
            dma((rows,)), dma((rows,)),
            dma((mates,)), dma((mates,)),
            dma((rows,)), dma((rows,)),
        ],
        compiler_params=pltpu.CompilerParams(collective_id=0, has_side_effects=True),
    )(returns, starts, start_block)


def gram_of(image):
    return jnp.einsum("wkj,wlj->wkl", image, image, precision=HIGHEST)


def project(factors, scaled):
    rounded = factors.astype(jnp.bfloat16)
    return jnp.einsum("wka,wta->wkt", rounded, scaled, preferred_element_type=jnp.float32)


def expand(proj, widened):
    return jnp.einsum("wkt,wta->wka", proj, widened, precision=HIGHEST)


def orthonormal(image, gram, assets):
    lower = jnp.linalg.cholesky(gram / assets)
    return jax.scipy.linalg.solve_triangular(lower, image, lower=True)


def stepwise(returns, starts, start_block, rows, mates):
    windows, days, width = returns.shape
    row_pos = lax.axis_index("rows")
    total_days = days * rows
    day_index = row_pos * days + jnp.arange(days, dtype=jnp.int32)
    live = (day_index[None, :, None] >= starts[:, None, :]).astype(jnp.float32)
    counts = (total_days - starts).astype(jnp.float32)
    masked = live * returns
    sums = lax.psum(jnp.sum(masked, axis=1), "rows")
    mean = sums / counts
    centered = live * (returns - mean[:, None, :])
    squares = lax.psum(jnp.sum(centered * centered, axis=1), "rows")
    scaled = (centered * lax.rsqrt(squares + 1.0)[:, None, :]).astype(jnp.bfloat16)
    widened = scaled.astype(jnp.float32)
    factors = start_block
    for step in range(ITERS):
        proj = lax.psum(project(factors, scaled), ("cols", "sub"))
        image = lax.psum(expand(proj, widened), "rows")
        gram = lax.psum(gram_of(image), ("cols", "sub"))
        factors = orthonormal(image, gram, width * mates)
    return factors


def on_device(rows, cols, subs, returns, starts, start_block):
    windows, days, width = returns.shape
    k = start_block.shape[1]
    fits = (windows == rows and width % (128 * rows) == 0 and days % 8 == 0 and k % 16 == 0
            and days * rows <= 64 and (days * rows + k) % 16 == 0 and rows > 1 and cols * subs > 1)
    if fits:
        return fused(returns, starts, start_block, rows, cols, subs)
    return stepwise(returns, starts, start_block, rows, cols * subs)


def solution(mesh):
    placed = (
        P("groups", "rows", ("cols", "sub")),
        P("groups", ("cols", "sub")),
        P("groups", None, ("cols", "sub")),
    )
    sizes = (mesh.shape["rows"], mesh.shape["cols"], mesh.shape["sub"])
    return jax.shard_map(
        functools.partial(on_device, *sizes),
        mesh=mesh,
        in_specs=placed,
        out_specs=P("groups", None, ("cols", "sub")),
        check_vma=False,
    )
```

```python
import functools

import jax
import jax.numpy as jnp
from jax import lax
from jax.experimental import pallas as pl
from jax.experimental.pallas import tpu as pltpu
from jax.sharding import PartitionSpec as P

ITERS = 3
HIGHEST = lax.Precision.HIGHEST
MESH = pl.DeviceIdType.MESH
NT = (((1,), (1,)), ((), ()))
SUBLANES = 8


def eliminate(gram, right):
    size = gram.shape[0]
    height = min(SUBLANES, size)
    blocks = size // height
    gs = [gram[b * height:(b + 1) * height] for b in range(blocks)]
    rs = [right[b * height:(b + 1) * height] for b in range(blocks)]
    row_id = lax.broadcasted_iota(jnp.int32, (height, 1), 0)
    diag = [jnp.ones((height, right.shape[1]), jnp.float32) for _ in range(blocks)]
    wide = max(size, right.shape[1])
    for b in range(blocks):
        panel = {
            (c, i): jnp.broadcast_to(gs[c][:, b * height + i:b * height + i + 1], (height, wide))
            for c in range(b, blocks) for i in range(height)
        }
        for i in range(height):
            grow = gs[b][i:i + 1]
            rrow = rs[b][i:i + 1]
            pivot = panel[b, i][i:i + 1]
            diag[b] = jnp.where(row_id == i, pivot[:, :right.shape[1]], diag[b])
            inverse = 1.0 / pivot
            ahead = {n: panel[b, n][i:i + 1] for n in range(i + 1, height)}
            for c in range(b, blocks):
                factor = panel[c, i] * inverse
                if c == b:
                    factor = jnp.where(row_id > i, factor, 0.0)
                for n in range(i + 1, height):
                    panel[c, n] = panel[c, n] - factor * ahead[n]
                gs[c] = gs[c] - factor[:, :size] * grow
                rs[c] = rs[c] - factor[:, :right.shape[1]] * rrow
    return jnp.concatenate([r * lax.rsqrt(d) for r, d in zip(rs, diag)], axis=0)


def kernel(rows, cols, subs, assets,
           returns_ref, starts_ref, start_ref, out_ref,
           held, begins, firsts, obuf, xbuf, sbuf, part, rs, mine, quad, mloc, mall,
           ls, bs, os, xs, xr, to_right, to_left, sr, ps, pr, qs, qr, ms, mr):
    r = lax.axis_index("rows")
    mates = cols * subs
    m = lax.axis_index("cols") * subs + lax.axis_index("sub")
    windows, days, width = returns_ref.shape
    k = start_ref.shape[1]
    total = days * rows
    own = width // rows
    half = (k + total) // 2

    def row_peer(d):
        return lax.rem(r + d, rows)

    def mate(d):
        return lax.rem(m + d, mates)

    def row_id(q):
        return {"rows": q}

    def mate_id(q):
        return {"cols": q // subs, "sub": lax.rem(q, subs)}

    def columns(q):
        return pl.ds(pl.multiple_of(q * own, own), own)

    loads = [pltpu.make_async_copy(returns_ref.at[w], held.at[w], ls.at[w]) for w in range(windows)]
    for c in loads:
        c.start()
    load_begins = pltpu.make_async_copy(starts_ref.at[:, columns(r)], begins, bs.at[0])
    load_begins.start()
    load_firsts = pltpu.make_async_copy(start_ref.at[:, :, columns(r)], firsts, bs.at[1])
    load_firsts.start()

    barrier = pltpu.get_barrier_semaphore()
    for d in range(1, rows):
        pl.semaphore_signal(barrier, inc=1, device_id=row_id(row_peer(d)), device_id_type=MESH)
    for d in range(1, mates):
        pl.semaphore_signal(barrier, inc=1, device_id=mate_id(mate(d)), device_id_type=MESH)
    pl.semaphore_wait(barrier, rows - 1 + mates - 1)

    def copy_to(src, dst, send, recv, target):
        return pltpu.make_async_remote_copy(
            src_ref=src, dst_ref=dst, send_sem=send, recv_sem=recv,
            device_id=target, device_id_type=MESH)

    sends = []
    for w in range(windows):
        loads[w].wait()
        for d in range(1, rows):
            q = row_peer(d)
            c = copy_to(held.at[w, :, columns(q)], xbuf.at[r, w], xs.at[w, d],
                        xr.at[w, r], row_id(q))
            c.start()
            sends.append(c)
    xbuf[r] = held[:, :, columns(r)]
    load_begins.wait()
    load_firsts.wait()

    def hop(q, w, right):
        sem = to_right if right else to_left
        target = row_id(lax.rem(r + (1 if right else rows - 1), rows))
        return copy_to(sbuf.at[q, w], sbuf.at[q, w], sem.at[q, w], sr.at[q, w], target)

    def hops(t, some, act):
        right_block = lax.rem(r - t + rows, rows)
        left_block = lax.rem(r + t, rows)
        for w in some:
            @pl.when(jnp.logical_and(r - t >= 0, r < rows - 1))
            def _():
                act(hop(right_block, w, True), t > 0)

            @pl.when(jnp.logical_and(r + t < rows, r > 0))
            def _():
                act(hop(left_block, w, False), t > 0)

    def forward(t, some):
        for w in some:
            if t > 0:
                @pl.when(r - t >= 0)
                def _():
                    hop(lax.rem(r - t + rows, rows), w, True).wait_recv()

                @pl.when(r + t < rows)
                def _():
                    hop(lax.rem(r + t, rows), w, True).wait_recv()
            hops(t, (w,), lambda c, _: c.start())

    def deliver(w):
        return copy_to(part.at[w], rs.at[r], ps.at[w], pr.at[r], row_id(w))

    ahead = windows // 2
    day = lax.broadcasted_iota(jnp.int32, (total, own), 0)
    for w in range(windows):
        for d in range(1, rows):
            q = row_peer(d)
            copy_to(held.at[w, :, columns(q)], xbuf.at[q, w], xs.at[w, d],
                    xr.at[w, q], row_id(q)).wait_recv()
        x = jnp.concatenate([xbuf[q, w] for q in range(rows)], axis=0)
        begin = begins[w:w + 1]
        live = day >= begin
        counts = (total - begin).astype(jnp.float32)
        mean = jnp.sum(jnp.where(live, x, 0.0), axis=0, keepdims=True) / counts
        centered = jnp.where(live, x - mean, 0.0)
        squares = jnp.sum(centered * centered, axis=0, keepdims=True)
        scaled = (centered * lax.rsqrt(squares + 1.0)).astype(jnp.bfloat16)
        sbuf[r, w] = scaled
        first = firsts[w].astype(jnp.bfloat16)
        sums = lax.dot_general(jnp.concatenate([first, scaled], axis=0), scaled, NT,
                               preferred_element_type=jnp.float32)
        part[w] = jnp.concatenate([sums[:half], sums[half:]], axis=1)

        @pl.when(r != w)
        def _():
            deliver(w).start()

        if w < ahead:
            forward(0, (w,))


    early, late = range(windows // 2), range(windows // 2, windows)
    schedule = [(t, some) for t in range(1, rows) for some in (early, late)]
    forward(0, range(ahead, windows))
    rs[r] = part[r]
    for d in range(1, rows):
        q = row_peer(d)
        copy_to(part.at[q], rs.at[q], ps.at[q], pr.at[q], row_id(q)).wait_recv()
    forward(*schedule.pop(0))
    summed = rs[0]
    for q in range(1, rows):
        summed = summed + rs[q]
    mine[...] = summed
    for d in range(1, mates):
        q = mate(d)
        c = copy_to(mine, quad.at[m], qs.at[d], qr.at[m], mate_id(q))
        c.start()
        sends.append(c)
    quad[m] = summed
    for d in range(1, mates):
        q = mate(d)
        copy_to(mine, quad.at[q], qs.at[d], qr.at[q], mate_id(q)).wait_recv()
    forward(*schedule.pop(0))
    both = quad[0]
    for q in range(1, mates):
        both = both + quad[q]
    both = jnp.concatenate([both[:, :total], both[:, total:]], axis=0)
    proj, corr = both[:k], both[k:]
    for step in range(ITERS):
        if step > 0 and len(schedule) > 2:
            forward(*schedule.pop(0))
        image = jnp.dot(proj, corr, precision=HIGHEST, preferred_element_type=jnp.float32)
        gram = lax.dot_general(image, proj, NT, precision=HIGHEST,
                               preferred_element_type=jnp.float32) / assets
        proj = eliminate(gram, image if step < ITERS - 1 else proj)
    mloc[...] = proj
    for d in range(1, rows):
        q = row_peer(d)
        c = copy_to(mloc, mall.at[r], ms.at[d], mr.at[r], row_id(q))
        c.start()
        sends.append(c)
    mall[r] = proj
    for entry in schedule:
        forward(*entry)
    for d in range(1, rows):
        q = row_peer(d)
        copy_to(mloc, mall.at[q], ms.at[d], mr.at[q], row_id(q)).wait_recv()
    stacked = []
    for w in range(windows):
        value = mall[w]
        high = value.astype(jnp.bfloat16)
        low = (value - high.astype(jnp.float32)).astype(jnp.bfloat16)
        stacked.append(jnp.concatenate([high, low], axis=0))

    def finish(q):
        for w in range(windows):
            wide = jnp.dot(stacked[w], sbuf[q, w], preferred_element_type=jnp.float32)
            obuf[q, w] = wide[:k] + wide[k:]
        c = pltpu.make_async_copy(obuf.at[q], out_ref.at[:, :, columns(q)], os.at[q])
        c.start()

    finish(r)
    for t in range(1, rows):
        for near in (True, False):
            @pl.when(r - t >= 0 if near else r + t < rows)
            def _():
                q = lax.rem(r - t + rows if near else r + t, rows)
                finish(q)
    for c in sends:
        c.wait_send()
    for w in range(windows):
        @pl.when(r != w)
        def _():
            deliver(w).wait_send()
    for t in range(rows):
        hops(t, range(windows), lambda c, _: c.wait_send())
    for q in range(rows):
        pltpu.make_async_copy(obuf.at[q], out_ref.at[:, :, columns(q)], os.at[q]).wait()


def fused(returns, starts, start_block, rows, cols, subs):
    windows, days, width = returns.shape
    k = start_block.shape[1]
    total = days * rows
    own = width // rows
    mates = cols * subs
    half = (k + total) // 2
    f32 = jnp.float32
    dma = pltpu.SemaphoreType.DMA
    return pl.pallas_call(
        functools.partial(kernel, rows, cols, subs, width * mates),
        out_shape=jax.ShapeDtypeStruct(start_block.shape, f32),
        in_specs=[pl.BlockSpec(memory_space=pl.ANY)] * 3,
        out_specs=pl.BlockSpec(memory_space=pl.ANY),
        scratch_shapes=[
            pltpu.VMEM(returns.shape, f32),
            pltpu.VMEM((windows, own), jnp.int32),
            pltpu.VMEM((windows, k, own), f32),
            pltpu.VMEM((rows, windows, k, own), f32),
            pltpu.VMEM((rows, windows, days, own), f32),
            pltpu.VMEM((rows, windows, total, own), jnp.bfloat16),
            pltpu.VMEM((windows, half, 2 * total), f32),
            pltpu.VMEM((rows, half, 2 * total), f32),
            pltpu.VMEM((half, 2 * total), f32),
            pltpu.VMEM((mates, half, 2 * total), f32),
            pltpu.VMEM((k, total), f32),
            pltpu.VMEM((windows, k, total), f32),
            dma((windows,)), dma((2,)), dma((rows,)),
            dma((windows, rows)), dma((windows, rows)),
            dma((rows, windows)), dma((rows, windows)), dma((rows, windows)),
            dma((rows,)), dma((rows,)),
            dma((mates,)), dma((mates,)),
            dma((rows,)), dma((rows,)),
        ],
        compiler_params=pltpu.CompilerParams(collective_id=0, has_side_effects=True),
    )(returns, starts, start_block)


def gram_of(image):
    return jnp.einsum("wkj,wlj->wkl", image, image, precision=HIGHEST)


def project(factors, scaled):
    rounded = factors.astype(jnp.bfloat16)
    return jnp.einsum("wka,wta->wkt", rounded, scaled, preferred_element_type=jnp.float32)


def expand(proj, widened):
    return jnp.einsum("wkt,wta->wka", proj, widened, precision=HIGHEST)


def orthonormal(image, gram, assets):
    lower = jnp.linalg.cholesky(gram / assets)
    return jax.scipy.linalg.solve_triangular(lower, image, lower=True)


def stepwise(returns, starts, start_block, rows, mates):
    windows, days, width = returns.shape
    row_pos = lax.axis_index("rows")
    total_days = days * rows
    day_index = row_pos * days + jnp.arange(days, dtype=jnp.int32)
    live = (day_index[None, :, None] >= starts[:, None, :]).astype(jnp.float32)
    counts = (total_days - starts).astype(jnp.float32)
    masked = live * returns
    sums = lax.psum(jnp.sum(masked, axis=1), "rows")
    mean = sums / counts
    centered = live * (returns - mean[:, None, :])
    squares = lax.psum(jnp.sum(centered * centered, axis=1), "rows")
    scaled = (centered * lax.rsqrt(squares + 1.0)[:, None, :]).astype(jnp.bfloat16)
    widened = scaled.astype(jnp.float32)
    factors = start_block
    for step in range(ITERS):
        proj = lax.psum(project(factors, scaled), ("cols", "sub"))
        image = lax.psum(expand(proj, widened), "rows")
        gram = lax.psum(gram_of(image), ("cols", "sub"))
        factors = orthonormal(image, gram, width * mates)
    return factors


def on_device(rows, cols, subs, returns, starts, start_block):
    windows, days, width = returns.shape
    k = start_block.shape[1]
    fits = (windows == rows and width % (128 * rows) == 0 and days % 8 == 0 and k % 16 == 0
            and days * rows <= 64 and (days * rows + k) % 16 == 0 and rows > 1 and cols * subs > 1)
    if fits:
        return fused(returns, starts, start_block, rows, cols, subs)
    return stepwise(returns, starts, start_block, rows, cols * subs)


def solution(mesh):
    placed = (
        P("groups", "rows", ("cols", "sub")),
        P("groups", ("cols", "sub")),
        P("groups", None, ("cols", "sub")),
    )
    sizes = (mesh.shape["rows"], mesh.shape["cols"], mesh.shape["sub"])
    return jax.shard_map(
        functools.partial(on_device, *sizes),
        mesh=mesh,
        in_specs=placed,
        out_specs=P("groups", None, ("cols", "sub")),
        check_vma=False,
    )
```
